32 devices in a mesh: vocab: 8 (over z, y), prompt: 4 (over x, core).
Axes of the slice: x: 2, y: 2, z: 4, core: 2. Of those that a mesh axis runs over, the one named last changes fastest.
Arguments:
- latent_vectors: bfloat16 [4096, 3584], P('prompt')
- unembedding_table: bfloat16 [3584, 81920], P('prompt', 'vocab'), may hold values from -0.3125 to 0.3125
- sampled_ids: int32 [4096], P('prompt'), may hold values from 0 to 81919
- query_of_reply: int32 [1024], P('prompt'), may hold values from 0 to 63, as said below
- critic_ratings: float32 [1024], P('prompt'), may hold values from -5 to 5
- initial_heat: float32 [64], P('prompt'), may hold values from 0.3 to 3
Outputs:
- sampled_logprob: float32 [4096], P('prompt')
- estep_factors: float32 [1024], P('prompt')
- temperature_out: float32 [64], P('prompt')
- weighted_nll: float32 [], replicated
The draws below stay inside these ranges and needn't reach their ends.
Inputs may be any that keep to these rules, and one draw needn't show every extreme that they name: Response r belongs to prompt query_of_reply[r]; every prompt has exactly 16 responses, all held by the same index of prompt as the prompt itself (the prompts of index i of prompt are i * 16 to i * 16 + 15), in any order there.
All inputs are finite; a program needn't handle non-finite values.
Results may differ from the reference program's by a relative error of at most 0.0003.
Values may be sent and summed in bfloat16 or wider, within the bound.
No kernel may reach another device: no remote copies, remote signals or barrier semaphores. Data moves between devices by JAX's collectives and lax.ppermute only.
A program may use at most 192 MiB of HBM per device.

```python
import math
import jax
import jax.numpy as jnp
import numpy as np
from jax import lax

D = 3584
V = 81920
REPLIES_EACH = 16
WIN = 4
NEWTON = 3
PROMPTS_PER_SHARD = 16
QUERY_TOTAL = 64
RESPONSES = 1024
TOKENS = 4096


def draw_query_of_reply(key, part):
    blocks = RESPONSES // (PROMPTS_PER_SHARD * REPLIES_EACH)
    local = jnp.repeat(jnp.arange(PROMPTS_PER_SHARD, dtype=jnp.int32), REPLIES_EACH)

    def one_block(index):
        mixed = jax.random.permutation(jax.random.fold_in(key, index), local)
        return mixed + index * PROMPTS_PER_SHARD
    return jax.vmap(one_block)(jnp.arange(blocks, dtype=jnp.int32)).reshape(RESPONSES).astype(jnp.int32)


def draw_latent_vectors(key, part):
    base = jax.random.normal(jax.random.fold_in(key, 11), (TOKENS, D), jnp.float32)
    return jnp.clip(base, -40.0, 40.0).astype(jnp.bfloat16)


def plant(result, own_key, least, high):
    spot = [jax.random.randint(jax.random.fold_in(own_key, axis), (), 0, length) for axis, length in enumerate(result.shape)]
    main_axis = result.shape.index(max(result.shape))
    next_to = spot[:main_axis] + [(spot[main_axis] + 1) % result.shape[main_axis]] + spot[main_axis + 1:]
    return result.at[tuple(spot)].set(least).at[tuple(next_to)].set(high)


def steps_of(stream_key, dims, split, smallest, high):
    def one(axis_at, blocks):
        heights = jax.random.uniform(jax.random.fold_in(jax.random.fold_in(stream_key, 6), axis_at), (blocks,), jnp.float32, smallest / len(split), high / len(split))
        return jnp.repeat(jnp.exp(heights), dims[axis_at] // blocks).reshape((-1,) + (1,) * (len(dims) - axis_at - 1))

    gain = one(*split[0])
    for cut in split[1:]:
        gain = gain * one(*cut)
    return gain


def skewed_wide(own_key, dims, number_of, slope):
    loads = [min(1 << octave, number_of + 1 - (1 << octave)) * (1 << 20) // math.isqrt((1 << octave) ** slope) + 1 for octave in range((number_of + 1).bit_length()) if 1 << octave <= number_of]
    spread = 1 + sum(loads) // (1 << 30)
    table = np.cumsum(np.array([max(1, weight // spread) for weight in loads]))
    lot = jax.random.randint(jax.random.fold_in(own_key, 1), dims, 0, int(table[len(loads) - 1]))
    start = jnp.left_shift(1, jnp.searchsorted(jnp.asarray(table, jnp.int32), lot, side="right").astype(jnp.int32))
    grade = start - 1 + jax.random.randint(jax.random.fold_in(own_key, 4), dims, 0, 1 << 30) % jnp.minimum(start, number_of + 1 - start)
    return jax.random.permutation(jax.random.fold_in(own_key, 2), number_of)[grade].astype(jnp.int32)


def noise(key, shape, scale, bound, shards=(), kind=jnp.bfloat16):
    loudness = steps_of(key, shape, shards, -0.22, 0.18) if shards else 1.0
    result = jax.random.normal(key, shape, jnp.float32) * scale * loudness
    return jnp.minimum(jnp.maximum(result, -bound), bound).astype(kind)


def setup_inputs(seed: int = 0) -> dict:
    key_of = jax.random.split(jax.random.key(seed), 7)
    latent_vectors = draw_latent_vectors(jax.random.fold_in(key_of[6], 71), 0)
    unembedding_table = noise(key_of[1], (D, V), (D // 9) ** -0.5, 0.3125, ((0, 4), (1, 8)))
    sampled_ids = plant(skewed_wide(key_of[2], (TOKENS,), V, 2), jax.random.fold_in(key_of[2], 3), 0, V - 1).astype(jnp.int32)
    query_of_reply = draw_query_of_reply(jax.random.fold_in(key_of[6], 71), 0)
    critic_ratings = noise(key_of[4], (RESPONSES,), 1.0, 5.0, ((0, 4),), jnp.float32)
    initial_heat = jnp.clip(jnp.exp(math.log(3.0) - 2.3025851 * jax.random.uniform(key_of[5], (QUERY_TOTAL,), jnp.float32) ** steps_of(key_of[5], (QUERY_TOTAL,), ((0, 4),), -0.2, 0.2)), 0.3, 3.0)
    return dict(latent_vectors=latent_vectors, unembedding_table=unembedding_table, sampled_ids=sampled_ids, query_of_reply=query_of_reply, critic_ratings=critic_ratings, initial_heat=initial_heat)


def token_block(hidden_rows, target_rows, unembedding_table):
    logits = jnp.dot(hidden_rows, unembedding_table, preferred_element_type=jnp.float32)
    largest = jnp.max(logits, axis=1)
    lse = largest + jnp.log(jnp.sum(jnp.exp(logits - largest[:, None]), axis=1))
    chosen = jnp.take_along_axis(logits, target_rows[:, None].astype(jnp.int32), axis=1)[:, 0]
    return chosen - lse


def fit_lagrange_heat(critic_ratings, sampled_onehot, initial_heat):
    masked = jnp.where(sampled_onehot > 0.5, critic_ratings[:, None], jnp.float32(-1e30))
    running_maximum = jnp.max(masked, axis=0)
    top_r = jnp.sum(sampled_onehot * running_maximum[None, :], axis=1)
    lagrange_heat = initial_heat
    for step in range(NEWTON):
        heat_of_reply = jnp.sum(sampled_onehot * lagrange_heat[None, :], axis=1)
        expo = jnp.exp((critic_ratings - top_r) / heat_of_reply)
        grand_accumulated = jnp.sum(sampled_onehot * expo[:, None], axis=0)
        share = expo / jnp.sum(sampled_onehot * grand_accumulated[None, :], axis=1)
        average_value = jnp.sum(sampled_onehot * (share * critic_ratings)[:, None], axis=0)
        mean_r = jnp.sum(sampled_onehot * average_value[None, :], axis=1)
        spread_queries = jnp.sum(sampled_onehot * (share * (critic_ratings - mean_r) ** 2)[:, None], axis=0)
        spread_queries = jnp.maximum(spread_queries, 0.1)
        first_derivative = 0.1 + jnp.log(grand_accumulated / REPLIES_EACH) + (running_maximum - average_value) / lagrange_heat
        second_derivative = spread_queries / lagrange_heat ** 3
        lagrange_heat = jnp.clip(lagrange_heat - first_derivative / second_derivative, 0.5 * lagrange_heat, 2.0 * lagrange_heat)
    heat_of_reply = jnp.sum(sampled_onehot * lagrange_heat[None, :], axis=1)
    expo = jnp.exp((critic_ratings - top_r) / heat_of_reply)
    grand_accumulated = jnp.sum(sampled_onehot * expo[:, None], axis=0)
    estep_factors = expo / jnp.sum(sampled_onehot * grand_accumulated[None, :], axis=1)
    return lagrange_heat, estep_factors


def reference(latent_vectors, unembedding_table, sampled_ids, query_of_reply, critic_ratings, initial_heat):
    rows = REPLIES_EACH * WIN
    hidden_blocks = latent_vectors.reshape(TOKENS // rows, rows, D)
    target_blocks = sampled_ids.reshape(TOKENS // rows, rows)
    sampled_logprob = lax.map(lambda pair: token_block(pair[0], pair[1], unembedding_table), (hidden_blocks, target_blocks)).reshape(TOKENS)
    resp_logp = jnp.sum(sampled_logprob.reshape(RESPONSES, WIN), axis=1)
    sampled_onehot = (query_of_reply[:, None] == jnp.arange(QUERY_TOTAL, dtype=jnp.int32)[None, :]).astype(jnp.float32)
    lagrange_heat, estep_factors = fit_lagrange_heat(critic_ratings, sampled_onehot, initial_heat)
    weighted_nll = -jnp.sum(estep_factors * resp_logp) / (QUERY_TOTAL * WIN)
    return sampled_logprob, estep_factors, lagrange_heat, weighted_nll
```

```python
import functools

import jax
import jax.numpy as jnp
from jax import lax
from jax.experimental import pallas as pl
from jax.experimental.pallas import tpu as pltpu
from jax.sharding import PartitionSpec as P


REPLIES_EACH = 16
WIN = 4
NEWTON = 3
PROMPTS_PER_SHARD = 16


LANES = 128
WIDTH = 512
ROWS = 512
CUTS = 4
EARLY = 2
VMEM_LIMIT = 60 * 1024 * 1024


def fit_lagrange_heat(critic_ratings, sampled_onehot, initial_heat):
    masked = jnp.where(sampled_onehot > 0.5, critic_ratings[:, None], jnp.float32(-1e30))
    running_maximum = jnp.max(masked, axis=0)
    top_r = jnp.sum(sampled_onehot * running_maximum[None, :], axis=1)
    lagrange_heat = initial_heat
    for _ in range(NEWTON):
        heat_of_reply = jnp.sum(sampled_onehot * lagrange_heat[None, :], axis=1)
        expo = jnp.exp((critic_ratings - top_r) / heat_of_reply)
        grand_accumulated = jnp.sum(sampled_onehot * expo[:, None], axis=0)
        share = expo / jnp.sum(sampled_onehot * grand_accumulated[None, :], axis=1)
        average_value = jnp.sum(sampled_onehot * (share * critic_ratings)[:, None], axis=0)
        mean_r = jnp.sum(sampled_onehot * average_value[None, :], axis=1)
        spread_queries = jnp.sum(
            sampled_onehot * (share * (critic_ratings - mean_r) ** 2)[:, None], axis=0
        )
        spread_queries = jnp.maximum(spread_queries, 0.1)
        first_derivative = (
            0.1
            + jnp.log(grand_accumulated / REPLIES_EACH)
            + (running_maximum - average_value) / lagrange_heat
        )
        second_derivative = spread_queries / lagrange_heat**3
        lagrange_heat = jnp.clip(
            lagrange_heat - first_derivative / second_derivative,
            0.5 * lagrange_heat,
            2.0 * lagrange_heat,
        )
    heat_of_reply = jnp.sum(sampled_onehot * lagrange_heat[None, :], axis=1)
    expo = jnp.exp((critic_ratings - top_r) / heat_of_reply)
    grand_accumulated = jnp.sum(sampled_onehot * expo[:, None], axis=0)
    estep_factors = expo / jnp.sum(sampled_onehot * grand_accumulated[None, :], axis=1)
    return (lagrange_heat, estep_factors)


def swap(value, axis, distance):
    size = lax.axis_size(axis)
    return lax.ppermute(value, axis, [(i, i ^ distance) for i in range(size)])


def shift(value, axis, distance):
    size = lax.axis_size(axis)
    return lax.ppermute(value, axis, [(i, (i + distance) % size) for i in range(size)])


def after(value, *others):
    return lax.optimization_barrier((value, *others))[0]


def cut_kernel(me_ref, *refs):
    count = len(refs) // 2
    for source, target in zip(refs[:count], refs[count:]):
        target[...] = source[...]


def cut_blocks(me, table, prompts, offset, width):
    rows = table.shape[0]
    quarter = table.shape[1] // prompts
    tall = rows // CUTS

    def piece(distance):
        return pl.BlockSpec(
            (tall, width),
            lambda i, me_ref: (i, ((me_ref[0] ^ distance) * quarter + offset) // width),
        )

    return pl.pallas_call(
        cut_kernel,
        grid_spec=pltpu.PrefetchScalarGridSpec(
            num_scalar_prefetch=1,
            grid=(CUTS,),
            in_specs=[piece(d) for d in range(1, prompts)],
            out_specs=[pl.BlockSpec((tall, width), lambda i, me_ref: (i, 0))] * (prompts - 1),
        ),
        out_shape=[jax.ShapeDtypeStruct((rows, width), table.dtype)] * (prompts - 1),
        cost_estimate=pl.CostEstimate(
            flops=rows * width, bytes_accessed=12 * rows * width, transcendentals=0
        ),
        name="cut",
    )(me, *([table] * (prompts - 1)))


def chunk_kernel(cfg, me_ref, place_ref, *refs):
    refs = list(refs)
    take = lambda count: [refs.pop(0) for _ in range(count)]
    distances, offset, quarter = cfg["distances"], cfg["offset"], cfg["quarter"]
    pieces = take(len(distances))
    tokens = take(cfg["tokens"])
    partial_ref = take(1)[0] if cfg["partial"] else None
    ids_ref = take(1)[0] if cfg["finish"] else None
    prior_ref = take(1)[0] if cfg["prior"] else None
    outs = take(cfg["outs"])
    weights, held, piece_sem, token_sem = take(4)
    first, second = take(2) if cfg["finish"] else (None, None)
    stats_ref = take(1)[0] if cfg["prior"] else (outs[0] if cfg["finish"] else None)
    before, before_sem = take(2) if cfg["partial"] else (None, None)

    step = pl.program_id(0)
    steps = cfg["steps"]
    me = me_ref[0]
    depth = pieces[-1].shape[0]
    width = weights.shape[1]
    tall = 2 * ROWS
    whole = len(distances) * depth == tokens[0].shape[1]

    strips = []
    for ref in tokens:
        high = min(ref.shape[0], tall)
        strips += [(ref, row, high) for row in range(0, ref.shape[0], high)]

    def copies(which):
        slot = which % 2
        found = []
        reached = 0
        start = which * tall
        for ref, row, high in strips:
            if start <= reached < start + tall:
                at = pl.ds(reached - start, high)
                if whole:
                    found.append((ref.at[pl.ds(row, high), :], held.at[slot, at, :]))
                else:
                    for index, distance in enumerate(distances):
                        owner = pl.multiple_of(lax.bitwise_xor(me, distance) * depth, depth)
                        found.append(
                            (
                                ref.at[pl.ds(row, high), pl.ds(owner, depth)],
                                held.at[slot, at, pl.ds(index * depth, depth)],
                            )
                        )
            reached += high
        made = [
            pltpu.make_async_copy(source, target, token_sem.at[slot, index])
            for index, (source, target) in enumerate(found)
        ]
        if partial_ref is not None:
            made.append(
                pltpu.make_async_copy(
                    partial_ref.at[pl.ds(start, tall), :], before.at[slot], before_sem.at[slot]
                )
            )
        return made

    def piece_copy(index):
        distance = distances[index]
        owner = lax.bitwise_xor(me, distance) if whole else index
        row = owner * depth
        target = weights.at[pl.ds(pl.multiple_of(row, depth) if whole else row, depth), :]
        source = pieces[index]
        if distance == 0:
            column = pl.multiple_of(me * quarter + offset, LANES)
            source = source.at[:, pl.ds(column, width)]
        return pltpu.make_async_copy(source, target, piece_sem.at[index])

    def finish(acc, tile):
        lane = lax.broadcasted_iota(jnp.int32, (LANES, LANES), 1)
        for part in range(ROWS // LANES):
            row = place_ref[tile * (ROWS // LANES) + part]
            logits = acc[part * LANES : (part + 1) * LANES, :]
            ids = ids_ref[pl.ds(pl.multiple_of(row * LANES, LANES), LANES), :]
            largest = jnp.max(logits, axis=1, keepdims=True)
            total = jnp.sum(jnp.exp(logits - largest), axis=1, keepdims=True)
            picked = jnp.zeros((LANES, LANES), jnp.float32)
            for block in range(width // LANES):
                hit = ids == lane + (offset + block * LANES)
                picked += jnp.where(hit, logits[:, block * LANES : (block + 1) * LANES], 0.0)
            chosen = jnp.sum(picked, axis=1, keepdims=True)
            packed = jnp.where(lane == 0, largest, jnp.where(lane == 1, total, chosen)).T
            for kind in range(3):
                stats_ref[kind, pl.ds(row, 1), :] = packed[kind : kind + 1, :]

    def product(slot, low):
        value = jnp.dot(
            held[slot, low : low + ROWS, :], weights[...], preferred_element_type=jnp.float32
        )
        return value if before is None else value + before[slot, low : low + ROWS, :]

    @pl.when(step == 0)
    def _():
        for copy in copies(0):
            copy.start()
        for index in range(len(distances)):
            piece_copy(index).start()
        if second is not None:
            second[...] = jnp.zeros_like(second)
        for index in range(len(distances)):
            piece_copy(index).wait()

    for which in range(steps):

        @pl.when(step == which)
        def _():
            if which + 1 < steps:
                for copy in copies(which + 1):
                    copy.start()
            for copy in copies(which):
                copy.wait()

    slot = lax.rem(step, 2)
    if not cfg["finish"]:
        outs[0][0:ROWS, :] = product(slot, 0)
        outs[0][ROWS:tall, :] = product(slot, ROWS)
        return

    first[...] = product(slot, 0)
    finish(second, jnp.maximum(2 * step - 1, 0))
    second[...] = product(slot, ROWS)
    finish(first, 2 * step)

    @pl.when(step == steps - 1)
    def _():
        finish(second, 2 * step + 1)
        if prior_ref is not None:
            each = prior_ref.shape[1] // len(outs)
            for index, out in enumerate(outs):
                rows = slice(index * each, (index + 1) * each)
                largest = jnp.maximum(stats_ref[0, rows, :], prior_ref[0, rows, :])
                out[0] = largest
                out[1] = stats_ref[1, rows, :] * jnp.exp(
                    stats_ref[0, rows, :] - largest
                ) + prior_ref[1, rows, :] * jnp.exp(prior_ref[0, rows, :] - largest)
                out[2] = stats_ref[2, rows, :] + prior_ref[2, rows, :]


def chunk_call(
    me, place, pieces, distances, tokens, quarter, offset, width, ids=None, partial=None,
    prior=None, parts=1
):
    count = sum(part.shape[0] for part in tokens)
    depth = pieces[-1].shape[0]
    inner = depth * len(distances)
    finish = ids is not None
    tall = 2 * ROWS
    steps = count // tall
    rows = count // LANES
    anywhere = pl.BlockSpec(memory_space=pl.ANY)
    whole = lambda shape: pl.BlockSpec(shape, lambda i, *_: (0,) * len(shape))
    operands = [*pieces, *tokens]
    in_specs = [anywhere] * len(operands)
    most = max(1, tall // min(part.shape[0] for part in tokens))
    scratch = [
        pltpu.VMEM((inner, width), tokens[0].dtype),
        pltpu.VMEM((2, tall, inner), tokens[0].dtype),
        pltpu.SemaphoreType.DMA((len(distances),)),
        pltpu.SemaphoreType.DMA((2, most * len(distances))),
    ]
    if partial is not None:
        operands.append(partial)
        in_specs.append(anywhere)
    if finish:
        operands.append(ids)
        in_specs.append(whole(ids.shape))
        scratch += [pltpu.VMEM((ROWS, width), jnp.float32)] * 2
    if prior is not None:
        operands.append(prior)
        in_specs.append(whole(prior.shape))
        scratch.append(pltpu.VMEM(prior.shape, jnp.float32))
        shape = (3, rows // parts, LANES)
        out_shape = [jax.ShapeDtypeStruct(shape, jnp.float32)] * parts
        out_specs = [whole(shape)] * parts
    elif finish:
        out_shape = [jax.ShapeDtypeStruct((3, rows, LANES), jnp.float32)]
        out_specs = [whole((3, rows, LANES))]
    else:
        out_shape = [jax.ShapeDtypeStruct((count, width), jnp.float32)]
        out_specs = [pl.BlockSpec((tall, width), lambda i, *_: (i, 0))]
    if partial is not None:
        scratch += [pltpu.VMEM((2, tall, width), jnp.float32), pltpu.SemaphoreType.DMA((2,))]
    cfg = dict(
        distances=distances,
        offset=offset,
        quarter=quarter,
        tokens=len(tokens),
        partial=partial is not None,
        finish=finish,
        prior=prior is not None,
        outs=len(out_shape),
        steps=steps,
    )
    return pl.pallas_call(
        functools.partial(chunk_kernel, cfg),
        grid_spec=pltpu.PrefetchScalarGridSpec(
            num_scalar_prefetch=2,
            grid=(steps,),
            in_specs=in_specs,
            out_specs=out_specs,
            scratch_shapes=scratch,
        ),
        out_shape=out_shape,
        compiler_params=pltpu.CompilerParams(
            dimension_semantics=("arbitrary",), vmem_limit_bytes=VMEM_LIMIT
        ),
        cost_estimate=pl.CostEstimate(
            flops=2 * count * inner * width,
            bytes_accessed=2 * inner * (count + width),
            transcendentals=count * width,
        ),
        name="chunk",
    )(me, place, *operands)


def tree(values):
    while len(values) > 1:
        pairs = [a + b for a, b in zip(values[::2], values[1::2])]
        values = pairs + values[2 * len(pairs) :]
    return values[0]


def merge(parts):
    largest = functools.reduce(jnp.maximum, [part[0] for part in parts])
    total = tree([part[1] * jnp.exp(part[0] - largest) for part in parts])
    chosen = tree([part[2] for part in parts])
    return jnp.stack([largest, total, chosen])


def all_pairs(value, axis):
    return [value] + [swap(value, axis, d) for d in range(1, lax.axis_size(axis))]


def exchange_stats(latent_vectors, unembedding_table, sampled_ids):
    prompts = lax.axis_size("prompt")
    vocabs = lax.axis_size("vocab")
    me = lax.axis_index("prompt").astype(jnp.int32)
    shard = lax.axis_index("vocab").astype(jnp.int32)
    each = latent_vectors.shape[0]
    columns = unembedding_table.shape[1]
    quarter = columns // prompts
    half = prompts // 2
    mine = me.reshape(1)
    chunks = quarter // WIDTH
    spans = list(range(prompts))

    strip = each // vocabs
    own = lax.dynamic_slice_in_dim(latent_vectors, shard * strip, strip, 0)
    over = swap(own, "prompt", half)
    partner = swap(latent_vectors, "prompt", 1)
    ids_all = [sampled_ids] + [swap(sampled_ids, "prompt", d) for d in range(1, prompts)]
    local = jnp.concatenate(ids_all) - (shard * columns + me * quarter)
    ids = jnp.broadcast_to(local[:, None], (each * prompts, LANES))

    cut = [
        cut_blocks(mine, unembedding_table, prompts, chunk * WIDTH, WIDTH)
        for chunk in range(chunks)
    ]
    pieces = []
    for blocks in cut:
        sent = [swap(block, "prompt", d + 1) for d, block in enumerate(blocks)]
        pieces.append([unembedding_table] + sent)

    ring = [after(over, *cut[0])]
    remote = []
    for hop in range(vocabs // 2):
        remote += [ring[-1], swap(ring[-1], "vocab", 1)]
        if hop + 1 < vocabs // 2:
            ring.append(shift(ring[-1], "vocab", 2))
    remote_pair = [swap(part, "prompt", 1) for part in remote]

    rows = strip // LANES
    order = []
    for hop in range(vocabs // 2):
        for other in (0, 1):
            origin = lax.rem((shard ^ other) - 2 * hop + vocabs, vocabs)
            order += [origin * rows + part for part in range(rows)]
    order = jnp.stack(order).astype(jnp.int32)
    near = jnp.arange(2 * each // LANES, dtype=jnp.int32)
    far = jnp.concatenate([order, order + each // LANES])
    place = jnp.concatenate([near, far + 2 * each // LANES])

    close, distant = [latent_vectors, partner], remote + remote_pair
    halves = ((near, close, ids[: 2 * each]), (far, distant, ids[2 * each :]))
    both = (place, close + distant, ids)
    early = min(EARLY, chunks - 1)
    jobs = [(chunk, half) for half in (0, 1) for chunk in range(early)]
    jobs += [(chunk, None) for chunk in range(early, chunks - 1)]
    done = {}
    gate = mine
    for chunk, half in jobs:
        where, tokens, part = both if half is None else halves[half]
        done[chunk, half] = chunk_call(
            gate, where, pieces[chunk], spans, tokens, quarter, chunk * WIDTH, WIDTH, ids=part
        )[0]
        gate = after(mine, done[chunk, half])
    prior = [jnp.concatenate([done[chunk, 0], done[chunk, 1]], axis=1) for chunk in range(early)]
    prior = merge(prior + [done[chunk, None] for chunk in range(early, chunks - 1)])
    offset = (chunks - 1) * WIDTH
    partial = chunk_call(
        gate, place, pieces[-1][: prompts - 1], spans[: prompts - 1], close + distant, quarter,
        offset, WIDTH,
    )[0]
    blocks = chunk_call(
        mine, place, pieces[-1][prompts - 1 :], spans[prompts - 1 :], close + distant, quarter,
        offset, WIDTH, ids=ids, partial=partial, prior=prior, parts=prompts,
    )
    return merge([block if d == 0 else swap(block, "prompt", d) for d, block in enumerate(blocks)])


def gather_stats(latent_vectors, unembedding_table, sampled_ids):
    columns = unembedding_table.shape[1]
    logits = jnp.dot(
        latent_vectors,
        lax.all_gather(unembedding_table, "prompt", axis=0, tiled=True),
        preferred_element_type=jnp.float32,
    )
    largest = jnp.max(logits, axis=1)
    total = jnp.sum(jnp.exp(logits - largest[:, None]), axis=1)
    local = sampled_ids - lax.axis_index("vocab") * columns
    positions = lax.broadcasted_iota(jnp.int32, (1, columns), 1)
    chosen = jnp.sum(jnp.where(positions == local[:, None], logits, 0.0), axis=1)
    return jnp.stack([largest, total, chosen]).reshape(3, -1, LANES)


def over_vocab(stats):
    size = lax.axis_size("vocab")
    if size <= 8:
        return merge(all_pairs(stats, "vocab"))
    distance = 1
    while distance < size:
        stats = merge([stats, swap(stats, "vocab", distance)])
        distance *= 2
    return stats


def shards(
    latent_vectors, unembedding_table, sampled_ids, query_of_reply, critic_ratings, initial_heat
):
    prompts = lax.axis_size("prompt")
    vocabs = lax.axis_size("vocab")
    each, columns = latent_vectors.shape[0], unembedding_table.shape[1]
    local_group = query_of_reply - lax.axis_index("prompt") * PROMPTS_PER_SHARD
    sampled_onehot = (
        local_group[:, None] == jnp.arange(PROMPTS_PER_SHARD, dtype=jnp.int32)[None, :]
    ).astype(jnp.float32)
    lagrange_heat, estep_factors = fit_lagrange_heat(critic_ratings, sampled_onehot, initial_heat)

    fits = (
        prompts == 4
        and vocabs % 2 == 0
        and columns % (prompts * WIDTH) == 0
        and columns > prompts * WIDTH
        and each % (2 * ROWS) == 0
        and each % (vocabs * LANES) == 0
    )
    partial = (exchange_stats if fits else gather_stats)(
        latent_vectors, unembedding_table, sampled_ids
    )
    whole_max, whole_sum, chosen = over_vocab(partial)
    sampled_logprob = chosen - (whole_max + jnp.log(whole_sum))
    spread_factors = jnp.repeat(estep_factors, WIN).reshape(sampled_logprob.shape)
    loss_part = jnp.sum(spread_factors * sampled_logprob)
    total_loss = tree(all_pairs(loss_part.reshape(1), "prompt"))[0]
    weighted_nll = -total_loss / (PROMPTS_PER_SHARD * prompts * WIN)
    return (sampled_logprob.reshape(-1), estep_factors, lagrange_heat, weighted_nll)


def solution(mesh):
    placed = (
        P("prompt", None),
        P("prompt", "vocab"),
        P("prompt"),
        P("prompt"),
        P("prompt"),
        P("prompt"),
    )
    return jax.shard_map(
        shards,
        mesh=mesh,
        in_specs=placed,
        out_specs=(P("prompt"), P("prompt"), P("prompt"), P()),
        check_vma=False,
    )
```

```python
import functools

import jax
import jax.numpy as jnp
from jax import lax
from jax.experimental import pallas as pl
from jax.experimental.pallas import tpu as pltpu
from jax.sharding import PartitionSpec as P


REPLIES_EACH = 16
WIN = 4
NEWTON = 3
PROMPTS_PER_SHARD = 16


LANES = 128
WIDTH = 512
ROWS = 256
SLOTS = 3
CUTS = 4
EARLY = 2
VMEM_LIMIT = 60 * 1024 * 1024


def fit_lagrange_heat(critic_ratings, sampled_onehot, initial_heat):
    masked = jnp.where(sampled_onehot > 0.5, critic_ratings[:, None], jnp.float32(-1e30))
    running_maximum = jnp.max(masked, axis=0)
    top_r = jnp.sum(sampled_onehot * running_maximum[None, :], axis=1)
    lagrange_heat = initial_heat
    for _ in range(NEWTON):
        heat_of_reply = jnp.sum(sampled_onehot * lagrange_heat[None, :], axis=1)
        expo = jnp.exp((critic_ratings - top_r) / heat_of_reply)
        grand_accumulated = jnp.sum(sampled_onehot * expo[:, None], axis=0)
        share = expo / jnp.sum(sampled_onehot * grand_accumulated[None, :], axis=1)
        average_value = jnp.sum(sampled_onehot * (share * critic_ratings)[:, None], axis=0)
        mean_r = jnp.sum(sampled_onehot * average_value[None, :], axis=1)
        spread_queries = jnp.sum(
            sampled_onehot * (share * (critic_ratings - mean_r) ** 2)[:, None], axis=0
        )
        spread_queries = jnp.maximum(spread_queries, 0.1)
        first_derivative = (
            0.1
            + jnp.log(grand_accumulated / REPLIES_EACH)
            + (running_maximum - average_value) / lagrange_heat
        )
        second_derivative = spread_queries / lagrange_heat**3
        lagrange_heat = jnp.clip(
            lagrange_heat - first_derivative / second_derivative,
            0.5 * lagrange_heat,
            2.0 * lagrange_heat,
        )
    heat_of_reply = jnp.sum(sampled_onehot * lagrange_heat[None, :], axis=1)
    expo = jnp.exp((critic_ratings - top_r) / heat_of_reply)
    grand_accumulated = jnp.sum(sampled_onehot * expo[:, None], axis=0)
    estep_factors = expo / jnp.sum(sampled_onehot * grand_accumulated[None, :], axis=1)
    return (lagrange_heat, estep_factors)


def swap(value, axis, distance):
    size = lax.axis_size(axis)
    return lax.ppermute(value, axis, [(i, i ^ distance) for i in range(size)])


def shift(value, axis, distance):
    size = lax.axis_size(axis)
    return lax.ppermute(value, axis, [(i, (i + distance) % size) for i in range(size)])


def after(value, *others):
    return lax.optimization_barrier((value, *others))[0]


def cut_kernel(me_ref, *refs):
    count = len(refs) // 2
    for source, target in zip(refs[:count], refs[count:]):
        target[...] = source[...]


def cut_blocks(me, table, prompts, offset, width):
    rows = table.shape[0]
    quarter = table.shape[1] // prompts
    tall = rows // CUTS

    def piece(distance):
        return pl.BlockSpec(
            (tall, width),
            lambda i, me_ref: (i, ((me_ref[0] ^ distance) * quarter + offset) // width),
        )

    return pl.pallas_call(
        cut_kernel,
        grid_spec=pltpu.PrefetchScalarGridSpec(
            num_scalar_prefetch=1,
            grid=(CUTS,),
            in_specs=[piece(d) for d in range(1, prompts)],
            out_specs=[pl.BlockSpec((tall, width), lambda i, me_ref: (i, 0))] * (prompts - 1),
        ),
        out_shape=[jax.ShapeDtypeStruct((rows, width), table.dtype)] * (prompts - 1),
        cost_estimate=pl.CostEstimate(
            flops=rows * width, bytes_accessed=12 * rows * width, transcendentals=0
        ),
        name="cut",
    )(me, *([table] * (prompts - 1)))


def chunk_kernel(cfg, me_ref, place_ref, *refs):
    refs = list(refs)
    take = lambda count: [refs.pop(0) for _ in range(count)]
    distances, offset, quarter = cfg["distances"], cfg["offset"], cfg["quarter"]
    pieces = take(len(distances))
    tokens = take(cfg["tokens"])
    partial_ref = take(1)[0] if cfg["partial"] else None
    ids_ref = take(1)[0] if cfg["finish"] else None
    prior_ref = take(1)[0] if cfg["prior"] else None
    outs = take(cfg["outs"])
    weights, held, piece_sem, token_sem = take(4)
    first, second = take(2) if cfg["finish"] else (None, None)
    stats_ref = take(1)[0] if cfg["prior"] else (outs[0] if cfg["finish"] else None)
    before, before_sem = take(2) if cfg["partial"] else (None, None)

    step = pl.program_id(0)
    steps = cfg["steps"]
    me = me_ref[0]
    depth = pieces[-1].shape[0]
    width = weights.shape[1]
    tall = 2 * ROWS
    whole = len(distances) * depth == tokens[0].shape[1]

    strips = []
    for ref in tokens:
        high = min(ref.shape[0], tall)
        strips += [(ref, row, high) for row in range(0, ref.shape[0], high)]

    def copies(which):
        slot = which % SLOTS
        found = []
        reached = 0
        start = which * tall
        for ref, row, high in strips:
            if start <= reached < start + tall:
                at = pl.ds(reached - start, high)
                if whole:
                    found.append((ref.at[pl.ds(row, high), :], held.at[slot, at, :]))
                else:
                    for index, distance in enumerate(distances):
                        owner = pl.multiple_of(lax.bitwise_xor(me, distance) * depth, depth)
                        found.append(
                            (
                                ref.at[pl.ds(row, high), pl.ds(owner, depth)],
                                held.at[slot, at, pl.ds(index * depth, depth)],
                            )
                        )
            reached += high
        made = [
            pltpu.make_async_copy(source, target, token_sem.at[slot, index])
            for index, (source, target) in enumerate(found)
        ]
        if partial_ref is not None:
            made.append(
                pltpu.make_async_copy(
                    partial_ref.at[pl.ds(start, tall), :], before.at[slot], before_sem.at[slot]
                )
            )
        return made

    def piece_copy(index):
        distance = distances[index]
        owner = lax.bitwise_xor(me, distance) if whole else index
        row = owner * depth
        target = weights.at[pl.ds(pl.multiple_of(row, depth) if whole else row, depth), :]
        source = pieces[index]
        if distance == 0:
            column = pl.multiple_of(me * quarter + offset, LANES)
            source = source.at[:, pl.ds(column, width)]
        return pltpu.make_async_copy(source, target, piece_sem.at[index])

    def finish(acc, tile):
        lane = lax.broadcasted_iota(jnp.int32, (LANES, LANES), 1)
        position = lane.astype(jnp.float32)
        for part in range(ROWS // LANES):
            row = place_ref[tile * (ROWS // LANES) + part]
            logits = acc[part * LANES : (part + 1) * LANES, :]
            ids = jnp.broadcast_to(ids_ref[pl.ds(row, 1), :], (LANES, LANES)).T
            largest = jnp.max(logits, axis=1, keepdims=True)
            total = jnp.sum(jnp.exp(logits - largest), axis=1, keepdims=True)
            picked = jnp.zeros((LANES, LANES), jnp.float32)
            for block in range(width // LANES):
                hit = ids == position + float(offset + block * LANES)
                picked += jnp.where(hit, logits[:, block * LANES : (block + 1) * LANES], 0.0)
            chosen = jnp.sum(picked, axis=1, keepdims=True)
            packed = jnp.where(lane == 0, largest, jnp.where(lane == 1, total, chosen)).T
            for kind in range(3):
                stats_ref[kind, pl.ds(row, 1), :] = packed[kind : kind + 1, :]

    def product(slot, low):
        value = jnp.dot(
            held[slot, low : low + ROWS, :], weights[...], preferred_element_type=jnp.float32
        )
        return value if before is None else value + before[slot, low : low + ROWS, :]

    @pl.when(step == 0)
    def _():
        for index in range(len(distances)):
            piece_copy(index).start()
        for ahead in range(min(SLOTS - 1, steps)):
            for copy in copies(ahead):
                copy.start()
        if second is not None:
            second[...] = jnp.zeros_like(second)
        for index in range(len(distances)):
            piece_copy(index).wait()

    for which in range(steps):

        @pl.when(step == which)
        def _():
            if which + SLOTS - 1 < steps:
                for copy in copies(which + SLOTS - 1):
                    copy.start()
            for copy in copies(which):
                copy.wait()

    slot = lax.rem(step, SLOTS)
    if not cfg["finish"]:
        outs[0][0:ROWS, :] = product(slot, 0)
        outs[0][ROWS:tall, :] = product(slot, ROWS)
        return

    first[...] = product(slot, 0)
    finish(second, jnp.maximum(2 * step - 1, 0))
    second[...] = product(slot, ROWS)
    finish(first, 2 * step)

    @pl.when(step == steps - 1)
    def _():
        finish(second, 2 * step + 1)
        if prior_ref is not None:
            each = prior_ref.shape[1] // len(outs)
            for index, out in enumerate(outs):
                rows = slice(index * each, (index + 1) * each)
                largest = jnp.maximum(stats_ref[0, rows, :], prior_ref[0, rows, :])
                out[0] = largest
                out[1] = stats_ref[1, rows, :] * jnp.exp(
                    stats_ref[0, rows, :] - largest
                ) + prior_ref[1, rows, :] * jnp.exp(prior_ref[0, rows, :] - largest)
                out[2] = stats_ref[2, rows, :] + prior_ref[2, rows, :]


def chunk_call(
    me, place, pieces, distances, tokens, quarter, offset, width, ids=None, partial=None,
    prior=None, parts=1
):
    count = sum(part.shape[0] for part in tokens)
    depth = pieces[-1].shape[0]
    inner = depth * len(distances)
    finish = ids is not None
    tall = 2 * ROWS
    steps = count // tall
    rows = count // LANES
    anywhere = pl.BlockSpec(memory_space=pl.ANY)
    whole = lambda shape: pl.BlockSpec(shape, lambda i, *_: (0,) * len(shape))
    operands = [*pieces, *tokens]
    in_specs = [anywhere] * len(operands)
    most = max(1, tall // min(part.shape[0] for part in tokens))
    scratch = [
        pltpu.VMEM((inner, width), tokens[0].dtype),
        pltpu.VMEM((SLOTS, tall, inner), tokens[0].dtype),
        pltpu.SemaphoreType.DMA((len(distances),)),
        pltpu.SemaphoreType.DMA((SLOTS, most * len(distances))),
    ]
    if partial is not None:
        operands.append(partial)
        in_specs.append(anywhere)
    if finish:
        operands.append(ids)
        in_specs.append(whole(ids.shape))
        scratch += [pltpu.VMEM((ROWS, width), jnp.float32)] * 2
    if prior is not None:
        operands.append(prior)
        in_specs.append(whole(prior.shape))
        scratch.append(pltpu.VMEM(prior.shape, jnp.float32))
        shape = (3, rows // parts, LANES)
        out_shape = [jax.ShapeDtypeStruct(shape, jnp.float32)] * parts
        out_specs = [whole(shape)] * parts
    elif finish:
        out_shape = [jax.ShapeDtypeStruct((3, rows, LANES), jnp.float32)]
        out_specs = [whole((3, rows, LANES))]
    else:
        out_shape = [jax.ShapeDtypeStruct((count, width), jnp.float32)]
        out_specs = [pl.BlockSpec((tall, width), lambda i, *_: (i, 0))]
    if partial is not None:
        scratch += [pltpu.VMEM((SLOTS, tall, width), jnp.float32), pltpu.SemaphoreType.DMA((SLOTS,))]
    cfg = dict(
        distances=distances,
        offset=offset,
        quarter=quarter,
        tokens=len(tokens),
        partial=partial is not None,
        finish=finish,
        prior=prior is not None,
        outs=len(out_shape),
        steps=steps,
    )
    return pl.pallas_call(
        functools.partial(chunk_kernel, cfg),
        grid_spec=pltpu.PrefetchScalarGridSpec(
            num_scalar_prefetch=2,
            grid=(steps,),
            in_specs=in_specs,
            out_specs=out_specs,
            scratch_shapes=scratch,
        ),
        out_shape=out_shape,
        compiler_params=pltpu.CompilerParams(
            dimension_semantics=("arbitrary",), vmem_limit_bytes=VMEM_LIMIT
        ),
        cost_estimate=pl.CostEstimate(
            flops=2 * count * inner * width,
            bytes_accessed=2 * inner * (count + width),
            transcendentals=count * width,
        ),
        name="chunk",
    )(me, place, *operands)


def tree(values):
    while len(values) > 1:
        pairs = [a + b for a, b in zip(values[::2], values[1::2])]
        values = pairs + values[2 * len(pairs) :]
    return values[0]


def merge(parts):
    largest = functools.reduce(jnp.maximum, [part[0] for part in parts])
    total = tree([part[1] * jnp.exp(part[0] - largest) for part in parts])
    chosen = tree([part[2] for part in parts])
    return jnp.stack([largest, total, chosen])


def all_pairs(value, axis):
    return [value] + [swap(value, axis, d) for d in range(1, lax.axis_size(axis))]


def exchange_stats(latent_vectors, unembedding_table, sampled_ids):
    prompts = lax.axis_size("prompt")
    vocabs = lax.axis_size("vocab")
    me = lax.axis_index("prompt").astype(jnp.int32)
    shard = lax.axis_index("vocab").astype(jnp.int32)
    each = latent_vectors.shape[0]
    columns = unembedding_table.shape[1]
    quarter = columns // prompts
    half = prompts // 2
    mine = me.reshape(1)
    chunks = quarter // WIDTH
    spans = list(range(prompts))

    strip = each // vocabs
    own = lax.dynamic_slice_in_dim(latent_vectors, shard * strip, strip, 0)
    over = swap(own, "prompt", half)
    partner = swap(latent_vectors, "prompt", 1)
    ids_all = [sampled_ids] + [swap(sampled_ids, "prompt", d) for d in range(1, prompts)]
    local = jnp.concatenate(ids_all) - (shard * columns + me * quarter)
    ids = local.astype(jnp.float32).reshape(-1, LANES)

    cut = [
        cut_blocks(mine, unembedding_table, prompts, chunk * WIDTH, WIDTH)
        for chunk in range(chunks)
    ]
    pieces = []
    for blocks in cut:
        sent = [swap(block, "prompt", d + 1) for d, block in enumerate(blocks)]
        pieces.append([unembedding_table] + sent)

    ring = [after(over, *cut[0])]
    remote = []
    for hop in range(vocabs // 2):
        remote += [ring[-1], swap(ring[-1], "vocab", 1)]
        if hop + 1 < vocabs // 2:
            ring.append(shift(ring[-1], "vocab", 2))
    remote_pair = [swap(part, "prompt", 1) for part in remote]

    rows = strip // LANES
    order = []
    for hop in range(vocabs // 2):
        for other in (0, 1):
            origin = lax.rem((shard ^ other) - 2 * hop + vocabs, vocabs)
            order += [origin * rows + part for part in range(rows)]
    order = jnp.stack(order).astype(jnp.int32)
    near = jnp.arange(2 * each // LANES, dtype=jnp.int32)
    far = jnp.concatenate([order, order + each // LANES])
    place = jnp.concatenate([near, far + 2 * each // LANES])

    close, distant = [latent_vectors, partner], remote + remote_pair
    halves = ((near, close, ids[: 2 * each // LANES]), (far, distant, ids[2 * each // LANES :]))
    both = (place, close + distant, ids)
    early = min(EARLY, chunks - 1)
    jobs = [(chunk, half) for half in (0, 1) for chunk in range(early)]
    jobs += [(chunk, None) for chunk in range(early, chunks - 1)]
    done = {}
    gate = mine
    for chunk, half in jobs:
        where, tokens, part = both if half is None else halves[half]
        done[chunk, half] = chunk_call(
            gate, where, pieces[chunk], spans, tokens, quarter, chunk * WIDTH, WIDTH, ids=part
        )[0]
        gate = after(mine, done[chunk, half])
    prior = [jnp.concatenate([done[chunk, 0], done[chunk, 1]], axis=1) for chunk in range(early)]
    prior = merge(prior + [done[chunk, None] for chunk in range(early, chunks - 1)])
    offset = (chunks - 1) * WIDTH
    partial = chunk_call(
        gate, place, pieces[-1][: prompts - 1], spans[: prompts - 1], close + distant, quarter,
        offset, WIDTH,
    )[0]
    blocks = chunk_call(
        mine, place, pieces[-1][prompts - 1 :], spans[prompts - 1 :], close + distant, quarter,
        offset, WIDTH, ids=ids, partial=partial, prior=prior, parts=prompts,
    )
    return merge([block if d == 0 else swap(block, "prompt", d) for d, block in enumerate(blocks)])


def gather_stats(latent_vectors, unembedding_table, sampled_ids):
    columns = unembedding_table.shape[1]
    logits = jnp.dot(
        latent_vectors,
        lax.all_gather(unembedding_table, "prompt", axis=0, tiled=True),
        preferred_element_type=jnp.float32,
    )
    largest = jnp.max(logits, axis=1)
    total = jnp.sum(jnp.exp(logits - largest[:, None]), axis=1)
    local = sampled_ids - lax.axis_index("vocab") * columns
    positions = lax.broadcasted_iota(jnp.int32, (1, columns), 1)
    chosen = jnp.sum(jnp.where(positions == local[:, None], logits, 0.0), axis=1)
    return jnp.stack([largest, total, chosen]).reshape(3, -1, LANES)


def over_vocab(stats):
    size = lax.axis_size("vocab")
    base = 1
    while base < size:
        radix = 2 if base == 1 else min(4, size // base)
        stats = merge(
            [stats] + [swap(stats, "vocab", base * digit) for digit in range(1, radix)]
        )
        base *= radix
    return stats


def shards(
    latent_vectors, unembedding_table, sampled_ids, query_of_reply, critic_ratings, initial_heat
):
    prompts = lax.axis_size("prompt")
    vocabs = lax.axis_size("vocab")
    each, columns = latent_vectors.shape[0], unembedding_table.shape[1]
    local_group = query_of_reply - lax.axis_index("prompt") * PROMPTS_PER_SHARD
    sampled_onehot = (
        local_group[:, None] == jnp.arange(PROMPTS_PER_SHARD, dtype=jnp.int32)[None, :]
    ).astype(jnp.float32)
    lagrange_heat, estep_factors = fit_lagrange_heat(critic_ratings, sampled_onehot, initial_heat)

    fits = (
        prompts == 4
        and vocabs % 2 == 0
        and columns % (prompts * WIDTH) == 0
        and columns > prompts * WIDTH
        and each % (2 * ROWS) == 0
        and each % (vocabs * LANES) == 0
    )
    partial = (exchange_stats if fits else gather_stats)(
        latent_vectors, unembedding_table, sampled_ids
    )
    whole_max, whole_sum, chosen = over_vocab(partial)
    sampled_logprob = chosen - (whole_max + jnp.log(whole_sum))
    spread_factors = jnp.repeat(estep_factors, WIN).reshape(sampled_logprob.shape)
    loss_part = jnp.sum(spread_factors * sampled_logprob)
    total_loss = tree(all_pairs(loss_part.reshape(1), "prompt"))[0]
    weighted_nll = -total_loss / (PROMPTS_PER_SHARD * prompts * WIN)
    return (sampled_logprob.reshape(-1), estep_factors, lagrange_heat, weighted_nll)


def solution(mesh):
    placed = (
        P("prompt", None),
        P("prompt", "vocab"),
        P("prompt"),
        P("prompt"),
        P("prompt"),
        P("prompt"),
    )
    return jax.shard_map(
        shards,
        mesh=mesh,
        in_specs=placed,
        out_specs=(P("prompt"), P("prompt"), P("prompt"), P()),
        check_vma=False,
    )
```

```python
import functools

import jax
import jax.numpy as jnp
from jax import lax
from jax.experimental import pallas as pl
from jax.experimental.pallas import tpu as pltpu
from jax.sharding import PartitionSpec as P


REPLIES_EACH = 16
WIN = 4
NEWTON = 3
PROMPTS_PER_SHARD = 16


LANES = 128
LOWEST = -3.0e38
WIDTH = 512
ROWS = 256
SLOTS = 3
CUTS = 4
EARLY = 2
VMEM_LIMIT = 60 * 1024 * 1024


def fit_lagrange_heat(critic_ratings, sampled_onehot, initial_heat):
    masked = jnp.where(sampled_onehot > 0.5, critic_ratings[:, None], jnp.float32(-1e30))
    running_maximum = jnp.max(masked, axis=0)
    top_r = jnp.sum(sampled_onehot * running_maximum[None, :], axis=1)
    lagrange_heat = initial_heat
    for _ in range(NEWTON):
        heat_of_reply = jnp.sum(sampled_onehot * lagrange_heat[None, :], axis=1)
        expo = jnp.exp((critic_ratings - top_r) / heat_of_reply)
        grand_accumulated = jnp.sum(sampled_onehot * expo[:, None], axis=0)
        share = expo / jnp.sum(sampled_onehot * grand_accumulated[None, :], axis=1)
        average_value = jnp.sum(sampled_onehot * (share * critic_ratings)[:, None], axis=0)
        mean_r = jnp.sum(sampled_onehot * average_value[None, :], axis=1)
        spread_queries = jnp.sum(
            sampled_onehot * (share * (critic_ratings - mean_r) ** 2)[:, None], axis=0
        )
        spread_queries = jnp.maximum(spread_queries, 0.1)
        first_derivative = (
            0.1
            + jnp.log(grand_accumulated / REPLIES_EACH)
            + (running_maximum - average_value) / lagrange_heat
        )
        second_derivative = spread_queries / lagrange_heat**3
        lagrange_heat = jnp.clip(
            lagrange_heat - first_derivative / second_derivative,
            0.5 * lagrange_heat,
            2.0 * lagrange_heat,
        )
    heat_of_reply = jnp.sum(sampled_onehot * lagrange_heat[None, :], axis=1)
    expo = jnp.exp((critic_ratings - top_r) / heat_of_reply)
    grand_accumulated = jnp.sum(sampled_onehot * expo[:, None], axis=0)
    estep_factors = expo / jnp.sum(sampled_onehot * grand_accumulated[None, :], axis=1)
    return (lagrange_heat, estep_factors)


def swap(value, axis, distance):
    size = lax.axis_size(axis)
    return lax.ppermute(value, axis, [(i, i ^ distance) for i in range(size)])


def shift(value, axis, distance):
    size = lax.axis_size(axis)
    return lax.ppermute(value, axis, [(i, (i + distance) % size) for i in range(size)])


def after(value, *others):
    return lax.optimization_barrier((value, *others))[0]


def cut_kernel(me_ref, *refs):
    count = len(refs) // 2
    for source, target in zip(refs[:count], refs[count:]):
        target[...] = source[...]


def cut_blocks(me, table, prompts, offset, width):
    rows = table.shape[0]
    quarter = table.shape[1] // prompts
    tall = rows // CUTS

    def piece(distance):
        return pl.BlockSpec(
            (tall, width),
            lambda i, me_ref: (i, ((me_ref[0] ^ distance) * quarter + offset) // width),
        )

    return pl.pallas_call(
        cut_kernel,
        grid_spec=pltpu.PrefetchScalarGridSpec(
            num_scalar_prefetch=1,
            grid=(CUTS,),
            in_specs=[piece(d) for d in range(1, prompts)],
            out_specs=[pl.BlockSpec((tall, width), lambda i, me_ref: (i, 0))] * (prompts - 1),
        ),
        out_shape=[jax.ShapeDtypeStruct((rows, width), table.dtype)] * (prompts - 1),
        cost_estimate=pl.CostEstimate(
            flops=rows * width, bytes_accessed=12 * rows * width, transcendentals=0
        ),
        name="cut",
    )(me, *([table] * (prompts - 1)))


def chunk_kernel(cfg, me_ref, place_ref, *refs):
    refs = list(refs)
    take = lambda count: [refs.pop(0) for _ in range(count)]
    distances, offset, quarter = cfg["distances"], cfg["offset"], cfg["quarter"]
    pieces = take(len(distances))
    tokens = take(cfg["tokens"])
    partial_ref = take(1)[0] if cfg["partial"] else None
    ids_ref = take(1)[0] if cfg["finish"] else None
    prior_ref = take(1)[0] if cfg["prior"] else None
    outs = take(cfg["outs"])
    weights, held, piece_sem, token_sem = take(4)
    first, second = take(2) if cfg["finish"] else (None, None)
    stats_ref = take(1)[0] if cfg["prior"] else (outs[0] if cfg["finish"] else None)
    before, before_sem = take(2) if cfg["partial"] else (None, None)

    step = pl.program_id(0)
    steps = cfg["steps"]
    me = me_ref[0]
    depth = pieces[-1].shape[0]
    width = weights.shape[1]
    tall = 2 * ROWS
    whole = len(distances) * depth == tokens[0].shape[1]

    strips = []
    for ref in tokens:
        high = min(ref.shape[0], tall)
        strips += [(ref, row, high) for row in range(0, ref.shape[0], high)]

    def copies(which):
        slot = which % SLOTS
        found = []
        reached = 0
        start = which * tall
        for ref, row, high in strips:
            if start <= reached < start + tall:
                at = pl.ds(reached - start, high)
                if whole:
                    found.append((ref.at[pl.ds(row, high), :], held.at[slot, at, :]))
                else:
                    for index, distance in enumerate(distances):
                        owner = pl.multiple_of(lax.bitwise_xor(me, distance) * depth, depth)
                        found.append(
                            (
                                ref.at[pl.ds(row, high), pl.ds(owner, depth)],
                                held.at[slot, at, pl.ds(index * depth, depth)],
                            )
                        )
            reached += high
        made = [
            pltpu.make_async_copy(source, target, token_sem.at[slot]) for source, target in found
        ]
        if partial_ref is not None:
            made.append(before_copy(which))
        return made

    def before_copy(which):
        slot = which % SLOTS
        return pltpu.make_async_copy(
            partial_ref.at[pl.ds(which * tall, tall), :], before.at[slot], before_sem.at[slot]
        )

    def landed(ref, sem):
        pltpu.make_async_copy(ref, ref, sem).wait()

    def piece_copy(index):
        distance = distances[index]
        owner = lax.bitwise_xor(me, distance) if whole else index
        row = owner * depth
        target = weights.at[pl.ds(pl.multiple_of(row, depth) if whole else row, depth), :]
        source = pieces[index]
        if distance == 0:
            column = pl.multiple_of(me * quarter + offset, LANES)
            source = source.at[:, pl.ds(column, width)]
        return pltpu.make_async_copy(source, target, piece_sem.at[0])

    def finish(acc, tile):
        lane = lax.broadcasted_iota(jnp.int32, (LANES, LANES), 1)
        position = lane.astype(jnp.float32)
        for part in range(ROWS // LANES):
            row = place_ref[tile * (ROWS // LANES) + part]
            logits = acc[part * LANES : (part + 1) * LANES, :]
            ids = jnp.broadcast_to(ids_ref[pl.ds(row, 1), :], (LANES, LANES)).T
            largest = jnp.max(logits, axis=1, keepdims=True)
            total = jnp.sum(jnp.exp(logits - largest), axis=1, keepdims=True)
            picked = jnp.zeros((LANES, LANES), jnp.float32)
            for block in range(width // LANES):
                hit = ids == position + float(offset + block * LANES)
                picked += jnp.where(hit, logits[:, block * LANES : (block + 1) * LANES], 0.0)
            chosen = jnp.sum(picked, axis=1, keepdims=True)
            packed = jnp.where(lane == 0, largest, jnp.where(lane == 1, total, chosen)).T
            for kind in range(3):
                stats_ref[kind, pl.ds(row, 1), :] = packed[kind : kind + 1, :]

    def product(slot, low):
        value = jnp.dot(
            held[slot, low : low + ROWS, :], weights[...], preferred_element_type=jnp.float32
        )
        return value if before is None else value + before[slot, low : low + ROWS, :]

    @pl.when(step == 0)
    def _():
        for index in range(len(distances)):
            piece_copy(index).start()
        for ahead in range(min(SLOTS - 1, steps)):
            for copy in copies(ahead):
                copy.start()
        if second is not None:
            second[...] = jnp.zeros_like(second)
            if prior_ref is None:
                neutral = jnp.zeros(stats_ref.shape[1:], jnp.float32)
                stats_ref[0] = neutral + LOWEST
                stats_ref[1] = neutral
                stats_ref[2] = neutral
        landed(weights, piece_sem.at[0])

    for which in range(steps):

        @pl.when(step == which)
        def _():
            if which + SLOTS - 1 < steps:
                for copy in copies(which + SLOTS - 1):
                    copy.start()
            landed(held.at[which % SLOTS], token_sem.at[which % SLOTS])
            if partial_ref is not None:
                before_copy(which).wait()

    slot = lax.rem(step, SLOTS)
    if not cfg["finish"]:
        outs[0][0:ROWS, :] = product(slot, 0)
        outs[0][ROWS:tall, :] = product(slot, ROWS)
        return

    first[...] = product(slot, 0)
    finish(second, jnp.maximum(2 * step - 1, 0))
    second[...] = product(slot, ROWS)
    finish(first, 2 * step)

    @pl.when(step == steps - 1)
    def _():
        finish(second, 2 * step + 1)
        if prior_ref is not None:
            each = prior_ref.shape[1] // len(outs)
            for index, out in enumerate(outs):
                rows = slice(index * each, (index + 1) * each)
                largest = jnp.maximum(stats_ref[0, rows, :], prior_ref[0, rows, :])
                out[0] = largest
                out[1] = stats_ref[1, rows, :] * jnp.exp(
                    stats_ref[0, rows, :] - largest
                ) + prior_ref[1, rows, :] * jnp.exp(prior_ref[0, rows, :] - largest)
                out[2] = stats_ref[2, rows, :] + prior_ref[2, rows, :]


def chunk_call(
    me, place, pieces, distances, tokens, quarter, offset, width, ids=None, partial=None,
    prior=None, parts=1
):
    count = sum(part.shape[0] for part in tokens)
    depth = pieces[-1].shape[0]
    inner = depth * len(distances)
    finish = ids is not None
    tall = 2 * ROWS
    steps = count // tall
    rows = count // LANES
    anywhere = pl.BlockSpec(memory_space=pl.ANY)
    whole = lambda shape: pl.BlockSpec(shape, lambda i, *_: (0,) * len(shape))
    operands = [*pieces, *tokens]
    in_specs = [anywhere] * len(operands)
    scratch = [
        pltpu.VMEM((inner, width), tokens[0].dtype),
        pltpu.VMEM((SLOTS, tall, inner), tokens[0].dtype),
        pltpu.SemaphoreType.DMA((1,)),
        pltpu.SemaphoreType.DMA((SLOTS,)),
    ]
    if partial is not None:
        operands.append(partial)
        in_specs.append(anywhere)
    if finish:
        operands.append(ids)
        in_specs.append(whole(ids.shape))
        scratch += [pltpu.VMEM((ROWS, width), jnp.float32)] * 2
    if prior is not None:
        operands.append(prior)
        in_specs.append(whole(prior.shape))
        scratch.append(pltpu.VMEM(prior.shape, jnp.float32))
        shape = (3, rows // parts, LANES)
        out_shape = [jax.ShapeDtypeStruct(shape, jnp.float32)] * parts
        out_specs = [whole(shape)] * parts
    elif finish:
        out_shape = [jax.ShapeDtypeStruct((3, *ids.shape), jnp.float32)]
        out_specs = [whole((3, *ids.shape))]
    else:
        out_shape = [jax.ShapeDtypeStruct((count, width), jnp.float32)]
        out_specs = [pl.BlockSpec((tall, width), lambda i, *_: (i, 0))]
    if partial is not None:
        scratch += [pltpu.VMEM((SLOTS, tall, width), jnp.float32), pltpu.SemaphoreType.DMA((SLOTS,))]
    cfg = dict(
        distances=distances,
        offset=offset,
        quarter=quarter,
        tokens=len(tokens),
        partial=partial is not None,
        finish=finish,
        prior=prior is not None,
        outs=len(out_shape),
        steps=steps,
    )
    return pl.pallas_call(
        functools.partial(chunk_kernel, cfg),
        grid_spec=pltpu.PrefetchScalarGridSpec(
            num_scalar_prefetch=2,
            grid=(steps,),
            in_specs=in_specs,
            out_specs=out_specs,
            scratch_shapes=scratch,
        ),
        out_shape=out_shape,
        compiler_params=pltpu.CompilerParams(
            dimension_semantics=("arbitrary",), vmem_limit_bytes=VMEM_LIMIT
        ),
        cost_estimate=pl.CostEstimate(
            flops=2 * count * inner * width,
            bytes_accessed=2 * inner * (count + width),
            transcendentals=count * width,
        ),
        name="chunk",
    )(me, place, *operands)


def tree(values):
    while len(values) > 1:
        pairs = [a + b for a, b in zip(values[::2], values[1::2])]
        values = pairs + values[2 * len(pairs) :]
    return values[0]


def merge(parts):
    largest = functools.reduce(jnp.maximum, [part[0] for part in parts])
    total = tree([part[1] * jnp.exp(part[0] - largest) for part in parts])
    chosen = tree([part[2] for part in parts])
    return jnp.stack([largest, total, chosen])


def all_pairs(value, axis):
    return [value] + [swap(value, axis, d) for d in range(1, lax.axis_size(axis))]


def exchange_stats(latent_vectors, unembedding_table, sampled_ids):
    prompts = lax.axis_size("prompt")
    vocabs = lax.axis_size("vocab")
    me = lax.axis_index("prompt").astype(jnp.int32)
    shard = lax.axis_index("vocab").astype(jnp.int32)
    each = latent_vectors.shape[0]
    columns = unembedding_table.shape[1]
    quarter = columns // prompts
    half = prompts // 2
    mine = me.reshape(1)
    chunks = quarter // WIDTH
    spans = list(range(prompts))

    strip = each // vocabs
    own = lax.dynamic_slice_in_dim(latent_vectors, shard * strip, strip, 0)
    over = swap(own, "prompt", half)
    partner = swap(latent_vectors, "prompt", 1)
    ids_all = [sampled_ids] + [swap(sampled_ids, "prompt", d) for d in range(1, prompts)]
    local = jnp.concatenate(ids_all) - (shard * columns + me * quarter)
    ids = local.astype(jnp.float32).reshape(-1, LANES)

    cut = [
        cut_blocks(mine, unembedding_table, prompts, chunk * WIDTH, WIDTH)
        for chunk in range(chunks)
    ]
    pieces = []
    for blocks in cut:
        sent = [swap(block, "prompt", d + 1) for d, block in enumerate(blocks)]
        pieces.append([unembedding_table] + sent)

    ring = [after(over, *cut[0])]
    remote = []
    for hop in range(vocabs // 2):
        remote += [ring[-1], swap(ring[-1], "vocab", 1)]
        if hop + 1 < vocabs // 2:
            ring.append(shift(ring[-1], "vocab", 2))
    remote_pair = [swap(part, "prompt", 1) for part in remote]

    rows = strip // LANES
    base = each // LANES

    def origins(hops):
        found = []
        for hop in hops:
            for other in (0, 1):
                origin = lax.rem((shard ^ other) - 2 * hop + vocabs, vocabs)
                found += [origin * rows + part for part in range(rows)]
        found = jnp.stack(found).astype(jnp.int32)
        return jnp.concatenate([found + half * base, found + (half + 1) * base])

    hops = vocabs // 2
    split = max(1, hops // 2)
    near = jnp.arange(2 * base, dtype=jnp.int32)
    soon = remote[: 2 * split] + remote_pair[: 2 * split]
    late = remote[2 * split :] + remote_pair[2 * split :]
    first = (jnp.concatenate([near, origins(range(split))]), [latent_vectors, partner] + soon)
    second = (origins(range(split, hops)), late)
    both = (jnp.concatenate([first[0], second[0]]), first[1] + second[1])

    early = min(EARLY, chunks - 1)
    gate = mine
    stats = []
    partial = None
    last = (chunks - 1) * WIDTH

    def head(distances, gate, partial):
        where, tokens = both
        return chunk_call(
            gate, where, [pieces[-1][d] for d in distances], distances, tokens, quarter, last, WIDTH,
            partial=partial,
        )[0]

    jobs = [(chunk, group) for group in (first, second) for chunk in range(early)]
    jobs += [(chunk, both) for chunk in range(early, chunks - 1)]
    for index, (chunk, (where, tokens)) in enumerate(jobs):
        if index == len(jobs) - 1:
            partial = head(spans[:half], gate, None)
            gate = after(mine, partial)
        found = chunk_call(
            gate, where, pieces[chunk], spans, tokens, quarter, chunk * WIDTH, WIDTH, ids=ids
        )[0]
        stats.append(found)
        gate = after(mine, found)
    for distance in spans[half:-1]:
        partial = head([distance], gate, partial)
    blocks = chunk_call(
        mine, both[0], pieces[-1][-1:], spans[-1:], both[1], quarter, last, WIDTH, ids=ids,
        partial=partial, prior=merge(stats), parts=prompts,
    )
    return merge([block if d == 0 else swap(block, "prompt", d) for d, block in enumerate(blocks)])


def gather_stats(latent_vectors, unembedding_table, sampled_ids):
    columns = unembedding_table.shape[1]
    logits = jnp.dot(
        latent_vectors,
        lax.all_gather(unembedding_table, "prompt", axis=0, tiled=True),
        preferred_element_type=jnp.float32,
    )
    largest = jnp.max(logits, axis=1)
    total = jnp.sum(jnp.exp(logits - largest[:, None]), axis=1)
    local = sampled_ids - lax.axis_index("vocab") * columns
    positions = lax.broadcasted_iota(jnp.int32, (1, columns), 1)
    chosen = jnp.sum(jnp.where(positions == local[:, None], logits, 0.0), axis=1)
    return jnp.stack([largest, total, chosen]).reshape(3, -1, LANES)


def over_vocab(stats):
    size = lax.axis_size("vocab")
    base = 1
    while base < size:
        radix = 2 if base == 1 else min(4, size // base)
        stats = merge(
            [stats] + [swap(stats, "vocab", base * digit) for digit in range(1, radix)]
        )
        base *= radix
    return stats


def shards(
    latent_vectors, unembedding_table, sampled_ids, query_of_reply, critic_ratings, initial_heat
):
    prompts = lax.axis_size("prompt")
    vocabs = lax.axis_size("vocab")
    each, columns = latent_vectors.shape[0], unembedding_table.shape[1]
    local_group = query_of_reply - lax.axis_index("prompt") * PROMPTS_PER_SHARD
    sampled_onehot = (
        local_group[:, None] == jnp.arange(PROMPTS_PER_SHARD, dtype=jnp.int32)[None, :]
    ).astype(jnp.float32)
    lagrange_heat, estep_factors = fit_lagrange_heat(critic_ratings, sampled_onehot, initial_heat)

    fits = (
        prompts == 4
        and vocabs % 2 == 0
        and columns % (prompts * WIDTH) == 0
        and columns > prompts * WIDTH
        and each % (2 * ROWS) == 0
        and each % (vocabs * LANES) == 0
    )
    partial = (exchange_stats if fits else gather_stats)(
        latent_vectors, unembedding_table, sampled_ids
    )
    whole_max, whole_sum, chosen = over_vocab(partial)
    sampled_logprob = chosen - (whole_max + jnp.log(whole_sum))
    spread_factors = jnp.repeat(estep_factors, WIN).reshape(sampled_logprob.shape)
    loss_part = jnp.sum(spread_factors * sampled_logprob)
    total_loss = tree(all_pairs(loss_part.reshape(1), "prompt"))[0]
    weighted_nll = -total_loss / (PROMPTS_PER_SHARD * prompts * WIN)
    return (sampled_logprob.reshape(-1), estep_factors, lagrange_heat, weighted_nll)


def solution(mesh):
    placed = (
        P("prompt", None),
        P("prompt", "vocab"),
        P("prompt"),
        P("prompt"),
        P("prompt"),
        P("prompt"),
    )
    return jax.shard_map(
        shards,
        mesh=mesh,
        in_specs=placed,
        out_specs=(P("prompt"), P("prompt"), P("prompt"), P()),
        check_vma=False,
    )
```

```python
import functools

import jax
import jax.numpy as jnp
from jax import lax
from jax.experimental import pallas as pl
from jax.experimental.pallas import tpu as pltpu
from jax.sharding import PartitionSpec as P


REPLIES_EACH = 16
WIN = 4
NEWTON = 3
PROMPTS_PER_SHARD = 16


LANES = 128
LOWEST = -3.0e38
WIDTH = 512
ROWS = 256
CUTS = 4
EARLY = 2
VMEM_LIMIT = 60 * 1024 * 1024


def fit_lagrange_heat(critic_ratings, sampled_onehot, initial_heat):
    masked = jnp.where(sampled_onehot > 0.5, critic_ratings[:, None], jnp.float32(-1e30))
    running_maximum = jnp.max(masked, axis=0)
    top_r = jnp.sum(sampled_onehot * running_maximum[None, :], axis=1)
    lagrange_heat = initial_heat
    for _ in range(NEWTON):
        heat_of_reply = jnp.sum(sampled_onehot * lagrange_heat[None, :], axis=1)
        expo = jnp.exp((critic_ratings - top_r) / heat_of_reply)
        grand_accumulated = jnp.sum(sampled_onehot * expo[:, None], axis=0)
        share = expo / jnp.sum(sampled_onehot * grand_accumulated[None, :], axis=1)
        average_value = jnp.sum(sampled_onehot * (share * critic_ratings)[:, None], axis=0)
        mean_r = jnp.sum(sampled_onehot * average_value[None, :], axis=1)
        spread_queries = jnp.sum(
            sampled_onehot * (share * (critic_ratings - mean_r) ** 2)[:, None], axis=0
        )
        spread_queries = jnp.maximum(spread_queries, 0.1)
        first_derivative = (
            0.1
            + jnp.log(grand_accumulated / REPLIES_EACH)
            + (running_maximum - average_value) / lagrange_heat
        )
        second_derivative = spread_queries / lagrange_heat**3
        lagrange_heat = jnp.clip(
            lagrange_heat - first_derivative / second_derivative,
            0.5 * lagrange_heat,
            2.0 * lagrange_heat,
        )
    heat_of_reply = jnp.sum(sampled_onehot * lagrange_heat[None, :], axis=1)
    expo = jnp.exp((critic_ratings - top_r) / heat_of_reply)
    grand_accumulated = jnp.sum(sampled_onehot * expo[:, None], axis=0)
    estep_factors = expo / jnp.sum(sampled_onehot * grand_accumulated[None, :], axis=1)
    return (lagrange_heat, estep_factors)


def swap(value, axis, distance):
    size = lax.axis_size(axis)
    return lax.ppermute(value, axis, [(i, i ^ distance) for i in range(size)])


def shift(value, axis, distance):
    size = lax.axis_size(axis)
    return lax.ppermute(value, axis, [(i, (i + distance) % size) for i in range(size)])


def after(value, *others):
    return lax.optimization_barrier((value, *others))[0]


def cut_kernel(me_ref, *refs):
    count = len(refs) // 2
    for source, target in zip(refs[:count], refs[count:]):
        target[...] = source[...]


def cut_blocks(me, table, prompts, offset, width):
    rows = table.shape[0]
    quarter = table.shape[1] // prompts
    tall = rows // CUTS

    def piece(distance):
        return pl.BlockSpec(
            (tall, width),
            lambda i, me_ref: (i, ((me_ref[0] ^ distance) * quarter + offset) // width),
        )

    return pl.pallas_call(
        cut_kernel,
        grid_spec=pltpu.PrefetchScalarGridSpec(
            num_scalar_prefetch=1,
            grid=(CUTS,),
            in_specs=[piece(d) for d in range(1, prompts)],
            out_specs=[pl.BlockSpec((tall, width), lambda i, me_ref: (i, 0))] * (prompts - 1),
        ),
        out_shape=[jax.ShapeDtypeStruct((rows, width), table.dtype)] * (prompts - 1),
        cost_estimate=pl.CostEstimate(
            flops=rows * width, bytes_accessed=12 * rows * width, transcendentals=0
        ),
        name="cut",
    )(me, *([table] * (prompts - 1)))


def chunk_kernel(cfg, me_ref, place_ref, *refs):
    refs = list(refs)
    take = lambda count: [refs.pop(0) for _ in range(count)]
    distances, offset, quarter = cfg["distances"], cfg["offset"], cfg["quarter"]
    pieces = take(len(distances))
    tokens = take(cfg["tokens"])
    partial_ref = take(1)[0] if cfg["partial"] else None
    ids_ref = take(1)[0] if cfg["finish"] else None
    prior_ref = take(1)[0] if cfg["prior"] else None
    outs = take(cfg["outs"])
    weights, held, piece_sem, token_sem = take(4)
    first, second = take(2) if cfg["finish"] else (None, None)
    stats_ref = take(1)[0] if cfg["prior"] else (outs[0] if cfg["finish"] else None)
    before, before_sem = take(2) if cfg["partial"] else (None, None)

    step = pl.program_id(0)
    steps, slots = cfg["steps"], cfg["slots"]
    me = me_ref[0]
    depth = pieces[-1].shape[0]
    width = weights.shape[1]
    tall = 2 * ROWS
    whole = len(distances) * depth == tokens[0].shape[1]

    strips = []
    for ref in tokens:
        high = min(ref.shape[0], tall)
        strips += [(ref, row, high) for row in range(0, ref.shape[0], high)]

    def copies(which):
        slot = which % slots
        found = []
        reached = 0
        start = which * tall
        for ref, row, high in strips:
            if start <= reached < start + tall:
                at = pl.ds(reached - start, high)
                if whole:
                    found.append((ref.at[pl.ds(row, high), :], held.at[slot, at, :]))
                else:
                    for index, distance in enumerate(distances):
                        owner = pl.multiple_of(lax.bitwise_xor(me, distance) * depth, depth)
                        found.append(
                            (
                                ref.at[pl.ds(row, high), pl.ds(owner, depth)],
                                held.at[slot, at, pl.ds(index * depth, depth)],
                            )
                        )
            reached += high
        made = [
            pltpu.make_async_copy(source, target, token_sem.at[slot]) for source, target in found
        ]
        if partial_ref is not None:
            made.append(before_copy(which))
        return made

    def before_copy(which):
        slot = which % slots
        return pltpu.make_async_copy(
            partial_ref.at[pl.ds(which * tall, tall), :], before.at[slot], before_sem.at[slot]
        )

    def landed(ref, sem):
        pltpu.make_async_copy(ref, ref, sem).wait()

    def piece_copy(index):
        distance = distances[index]
        owner = lax.bitwise_xor(me, distance) if whole else index
        row = owner * depth
        target = weights.at[pl.ds(pl.multiple_of(row, depth) if whole else row, depth), :]
        source = pieces[index]
        if distance == 0:
            column = pl.multiple_of(me * quarter + offset, LANES)
            source = source.at[:, pl.ds(column, width)]
        return pltpu.make_async_copy(source, target, piece_sem.at[0])

    def finish(acc, tile):
        lane = lax.broadcasted_iota(jnp.int32, (LANES, LANES), 1)
        position = lane.astype(jnp.float32)
        for part in range(ROWS // LANES):
            row = place_ref[tile * (ROWS // LANES) + part]
            logits = acc[part * LANES : (part + 1) * LANES, :]
            ids = jnp.broadcast_to(ids_ref[pl.ds(row, 1), :], (LANES, LANES)).T
            largest = jnp.max(logits, axis=1, keepdims=True)
            total = jnp.sum(jnp.exp(logits - largest), axis=1, keepdims=True)
            picked = jnp.zeros((LANES, LANES), jnp.float32)
            for block in range(width // LANES):
                hit = ids == position + float(offset + block * LANES)
                picked += jnp.where(hit, logits[:, block * LANES : (block + 1) * LANES], 0.0)
            chosen = jnp.sum(picked, axis=1, keepdims=True)
            packed = jnp.where(lane == 0, largest, jnp.where(lane == 1, total, chosen)).T
            for kind in range(3):
                stats_ref[kind, pl.ds(row, 1), :] = packed[kind : kind + 1, :]

    def product(slot, low):
        value = jnp.dot(
            held[slot, low : low + ROWS, :], weights[...], preferred_element_type=jnp.float32
        )
        return value if before is None else value + before[slot, low : low + ROWS, :]

    @pl.when(step == 0)
    def _():
        for index in range(len(distances)):
            piece_copy(index).start()
        for ahead in range(min(slots - 1, steps)):
            for copy in copies(ahead):
                copy.start()
        if second is not None:
            second[...] = jnp.zeros_like(second)
            if prior_ref is None:
                neutral = jnp.zeros(stats_ref.shape[1:], jnp.float32)
                stats_ref[0] = neutral + LOWEST
                stats_ref[1] = neutral
                stats_ref[2] = neutral
        landed(weights, piece_sem.at[0])

    for which in range(steps):

        @pl.when(step == which)
        def _():
            if which + slots - 1 < steps:
                for copy in copies(which + slots - 1):
                    copy.start()
            landed(held.at[which % slots], token_sem.at[which % slots])
            if partial_ref is not None:
                before_copy(which).wait()

    slot = lax.rem(step, slots)
    if not cfg["finish"]:
        outs[0][0:ROWS, :] = product(slot, 0)
        outs[0][ROWS:tall, :] = product(slot, ROWS)
        return

    first[...] = product(slot, 0)
    finish(second, jnp.maximum(2 * step - 1, 0))
    second[...] = product(slot, ROWS)
    finish(first, 2 * step)

    @pl.when(step == steps - 1)
    def _():
        finish(second, 2 * step + 1)
        if prior_ref is not None:
            each = prior_ref.shape[1] // len(outs)
            for index, out in enumerate(outs):
                rows = slice(index * each, (index + 1) * each)
                largest = jnp.maximum(stats_ref[0, rows, :], prior_ref[0, rows, :])
                out[0] = largest
                out[1] = stats_ref[1, rows, :] * jnp.exp(
                    stats_ref[0, rows, :] - largest
                ) + prior_ref[1, rows, :] * jnp.exp(prior_ref[0, rows, :] - largest)
                out[2] = stats_ref[2, rows, :] + prior_ref[2, rows, :]


def chunk_call(
    me, place, pieces, distances, tokens, quarter, offset, width, ids=None, partial=None,
    prior=None, parts=1
):
    count = sum(part.shape[0] for part in tokens)
    depth = pieces[-1].shape[0]
    inner = depth * len(distances)
    finish = ids is not None
    tall = 2 * ROWS
    steps = count // tall
    slots = 2 if partial is None else 3
    rows = count // LANES
    anywhere = pl.BlockSpec(memory_space=pl.ANY)
    whole = lambda shape: pl.BlockSpec(shape, lambda i, *_: (0,) * len(shape))
    operands = [*pieces, *tokens]
    in_specs = [anywhere] * len(operands)
    scratch = [
        pltpu.VMEM((inner, width), tokens[0].dtype),
        pltpu.VMEM((slots, tall, inner), tokens[0].dtype),
        pltpu.SemaphoreType.DMA((1,)),
        pltpu.SemaphoreType.DMA((slots,)),
    ]
    if partial is not None:
        operands.append(partial)
        in_specs.append(anywhere)
    if finish:
        operands.append(ids)
        in_specs.append(whole(ids.shape))
        scratch += [pltpu.VMEM((ROWS, width), jnp.float32)] * 2
    if prior is not None:
        operands.append(prior)
        in_specs.append(whole(prior.shape))
        scratch.append(pltpu.VMEM(prior.shape, jnp.float32))
        shape = (3, rows // parts, LANES)
        out_shape = [jax.ShapeDtypeStruct(shape, jnp.float32)] * parts
        out_specs = [whole(shape)] * parts
    elif finish:
        out_shape = [jax.ShapeDtypeStruct((3, *ids.shape), jnp.float32)]
        out_specs = [whole((3, *ids.shape))]
    else:
        out_shape = [jax.ShapeDtypeStruct((count, width), jnp.float32)]
        out_specs = [pl.BlockSpec((tall, width), lambda i, *_: (i, 0))]
    if partial is not None:
        scratch += [pltpu.VMEM((slots, tall, width), jnp.float32), pltpu.SemaphoreType.DMA((slots,))]
    cfg = dict(
        distances=distances,
        offset=offset,
        quarter=quarter,
        tokens=len(tokens),
        partial=partial is not None,
        finish=finish,
        prior=prior is not None,
        outs=len(out_shape),
        steps=steps,
        slots=slots,
    )
    return pl.pallas_call(
        functools.partial(chunk_kernel, cfg),
        grid_spec=pltpu.PrefetchScalarGridSpec(
            num_scalar_prefetch=2,
            grid=(steps,),
            in_specs=in_specs,
            out_specs=out_specs,
            scratch_shapes=scratch,
        ),
        out_shape=out_shape,
        compiler_params=pltpu.CompilerParams(
            dimension_semantics=("arbitrary",), vmem_limit_bytes=VMEM_LIMIT
        ),
        cost_estimate=pl.CostEstimate(
            flops=2 * count * inner * width,
            bytes_accessed=2 * inner * (count + width),
            transcendentals=count * width,
        ),
        name="chunk",
    )(me, place, *operands)


def tree(values):
    while len(values) > 1:
        pairs = [a + b for a, b in zip(values[::2], values[1::2])]
        values = pairs + values[2 * len(pairs) :]
    return values[0]


def merge(parts):
    largest = functools.reduce(jnp.maximum, [part[0] for part in parts])
    total = tree([part[1] * jnp.exp(part[0] - largest) for part in parts])
    chosen = tree([part[2] for part in parts])
    return jnp.stack([largest, total, chosen])


def all_pairs(value, axis):
    return [value] + [swap(value, axis, d) for d in range(1, lax.axis_size(axis))]


def exchange_stats(latent_vectors, unembedding_table, sampled_ids):
    prompts = lax.axis_size("prompt")
    vocabs = lax.axis_size("vocab")
    me = lax.axis_index("prompt").astype(jnp.int32)
    shard = lax.axis_index("vocab").astype(jnp.int32)
    each = latent_vectors.shape[0]
    columns = unembedding_table.shape[1]
    quarter = columns // prompts
    half = prompts // 2
    mine = me.reshape(1)
    chunks = quarter // WIDTH
    spans = list(range(prompts))

    strip = each // vocabs
    own = lax.dynamic_slice_in_dim(latent_vectors, shard * strip, strip, 0)
    over = swap(own, "prompt", half)
    partner = swap(latent_vectors, "prompt", 1)
    ids_all = [sampled_ids] + [swap(sampled_ids, "prompt", d) for d in range(1, prompts)]
    local = jnp.concatenate(ids_all) - (shard * columns + me * quarter)
    ids = local.astype(jnp.float32).reshape(-1, LANES)

    cut = []
    for chunk in range(chunks):
        cut.append(cut_blocks(mine, unembedding_table, prompts, chunk * WIDTH, WIDTH))
    pieces = []
    for blocks in cut:
        sent = [swap(block, "prompt", d + 1) for d, block in enumerate(blocks)]
        pieces.append([unembedding_table] + sent)

    ring = [after(over, *cut[0])]
    remote = []
    for hop in range(vocabs // 2):
        remote += [ring[-1], swap(ring[-1], "vocab", 1)]
        if hop + 1 < vocabs // 2:
            ring.append(shift(ring[-1], "vocab", 2))
    remote_pair = []
    for part in remote:
        remote_pair.append(swap(part, "prompt", 1))

    rows = strip // LANES
    base = each // LANES

    def origins(hops):
        found = []
        for hop in hops:
            for other in (0, 1):
                origin = lax.rem((shard ^ other) - 2 * hop + vocabs, vocabs)
                found += [origin * rows + part for part in range(rows)]
        found = jnp.stack(found).astype(jnp.int32)
        return jnp.concatenate([found + half * base, found + (half + 1) * base])

    hops = vocabs // 2
    split = max(1, hops // 2)
    near = jnp.arange(2 * base, dtype=jnp.int32)
    soon = remote[: 2 * split] + remote_pair[: 2 * split]
    late = remote[2 * split :] + remote_pair[2 * split :]
    first = (jnp.concatenate([near, origins(range(split))]), [latent_vectors, partner] + soon)
    second = (origins(range(split, hops)), late)
    both = (jnp.concatenate([first[0], second[0]]), first[1] + second[1])

    early = min(EARLY, chunks - 1)
    gate = mine
    stats = []
    partial = None
    last = (chunks - 1) * WIDTH

    def head(distances, gate, partial):
        where, tokens = both
        return chunk_call(
            gate, where, [pieces[-1][d] for d in distances], distances, tokens, quarter, last, WIDTH,
            partial=partial,
        )[0]

    jobs = [(chunk, group) for group in (first, second) for chunk in range(early)]
    jobs += [(chunk, both) for chunk in range(early, chunks - 1)]
    for index, (chunk, (where, tokens)) in enumerate(jobs):
        if index == len(jobs) - 1:
            partial = head(spans[:half], gate, None)
            gate = after(mine, partial)
        found = chunk_call(
            gate, where, pieces[chunk], spans, tokens, quarter, chunk * WIDTH, WIDTH, ids=ids
        )[0]
        stats.append(found)
        gate = after(mine, found)
    for distance in spans[half:-1]:
        partial = head([distance], gate, partial)
    blocks = chunk_call(
        mine, both[0], pieces[-1][-1:], spans[-1:], both[1], quarter, last, WIDTH, ids=ids,
        partial=partial, prior=merge(stats), parts=prompts,
    )
    return merge([block if d == 0 else swap(block, "prompt", d) for d, block in enumerate(blocks)])


def gather_stats(latent_vectors, unembedding_table, sampled_ids):
    columns = unembedding_table.shape[1]
    logits = jnp.dot(
        latent_vectors,
        lax.all_gather(unembedding_table, "prompt", axis=0, tiled=True),
        preferred_element_type=jnp.float32,
    )
    largest = jnp.max(logits, axis=1)
    total = jnp.sum(jnp.exp(logits - largest[:, None]), axis=1)
    local = sampled_ids - lax.axis_index("vocab") * columns
    positions = lax.broadcasted_iota(jnp.int32, (1, columns), 1)
    chosen = jnp.sum(jnp.where(positions == local[:, None], logits, 0.0), axis=1)
    return jnp.stack([largest, total, chosen]).reshape(3, -1, LANES)


def over_vocab(stats):
    size = lax.axis_size("vocab")
    base = 1
    while base < size:
        radix = min(4, size // base)
        stats = merge(
            [stats] + [swap(stats, "vocab", base * digit) for digit in range(1, radix)]
        )
        base *= radix
    return stats


def shards(
    latent_vectors, unembedding_table, sampled_ids, query_of_reply, critic_ratings, initial_heat
):
    prompts = lax.axis_size("prompt")
    vocabs = lax.axis_size("vocab")
    each, columns = latent_vectors.shape[0], unembedding_table.shape[1]
    local_group = query_of_reply - lax.axis_index("prompt") * PROMPTS_PER_SHARD
    sampled_onehot = (
        local_group[:, None] == jnp.arange(PROMPTS_PER_SHARD, dtype=jnp.int32)[None, :]
    ).astype(jnp.float32)
    lagrange_heat, estep_factors = fit_lagrange_heat(critic_ratings, sampled_onehot, initial_heat)

    fits = (
        prompts == 4
        and vocabs % 2 == 0
        and columns % (prompts * WIDTH) == 0
        and columns > prompts * WIDTH
        and each % (2 * ROWS) == 0
        and each % (vocabs * LANES) == 0
    )
    partial = (exchange_stats if fits else gather_stats)(
        latent_vectors, unembedding_table, sampled_ids
    )
    whole_max, whole_sum, chosen = over_vocab(partial)
    sampled_logprob = chosen - (whole_max + jnp.log(whole_sum))
    spread_factors = jnp.repeat(estep_factors, WIN).reshape(sampled_logprob.shape)
    loss_part = jnp.sum(spread_factors * sampled_logprob)
    total_loss = tree(all_pairs(loss_part.reshape(1), "prompt"))[0]
    weighted_nll = -total_loss / (PROMPTS_PER_SHARD * prompts * WIN)
    return (sampled_logprob.reshape(-1), estep_factors, lagrange_heat, weighted_nll)


def solution(mesh):
    placed = (
        P("prompt", None),
        P("prompt", "vocab"),
        P("prompt"),
        P("prompt"),
        P("prompt"),
        P("prompt"),
    )
    return jax.shard_map(
        shards,
        mesh=mesh,
        in_specs=placed,
        out_specs=(P("prompt"), P("prompt"), P("prompt"), P()),
        check_vma=False,
    )
```
